32 devices in a mesh: pass: 4 (over y, x), red: 4 (over z), grp: 2 (over core).
Axes of the slice: x: 2, y: 2, z: 4, core: 2. Of those that a mesh axis runs over, the one named last changes fastest.
Arguments:
- query_lex: bfloat16 [1536, 16384], P(None, 'red')
- query_dense: bfloat16 [1536, 4096], P(None, 'red')
- passage_lex: bfloat16 [4096, 16384], P(('pass', 'grp'), 'red'), may hold values from 0 to 0.47
- passage_dense: bfloat16 [4096, 4096], P(('pass', 'grp'), 'red'), may hold values from -1.33 to 1.33
- positives: int32 [1536], replicated, may hold values from 0 to 4095
Outputs:
- loss_rows: float32 [1536], P('red')
- grad_query_lex: float32 [1536, 16384], P(('pass', 'grp'), 'red')
- grad_query_dense: float32 [1536, 4096], P(('pass', 'grp'), 'red')
- grad_passage_lex: float32 [4096, 16384], P(('pass', 'grp'), 'red')
- grad_passage_dense: float32 [4096, 4096], P(('pass', 'grp'), 'red')
The draws below stay inside these ranges and needn't reach their ends.
All inputs are finite; a program needn't handle non-finite values.
Results may differ from the reference program's by a relative error of at most 0.0022.
Values may be sent and summed in bfloat16 or wider, within the bound.
A program may use at most 192 MiB of HBM per device.

```python
import jax
import jax.numpy as jnp
from jax import lax

VOCAB = 16384
WIDTH = 4096
QUERIES = 1536
PASSAGES = 4096


lex_scale = 0.46


dense_scale = 0.177


def lexical_row(base, index):
    row_key = jax.random.fold_in(base, index)
    mask_key, value_key = jax.random.split(row_key)
    present = jax.random.bernoulli(mask_key, 0.25, (VOCAB,)).astype(jnp.float32)
    values = jax.random.uniform(value_key, (VOCAB,), jnp.float32)
    ramp = 1.0 + 0.02 * index.astype(jnp.float32) / PASSAGES
    return present * values * lex_scale * ramp


def dense_row(base, index):
    row_key = jax.random.fold_in(base, index)
    value_key = jax.random.fold_in(row_key, 0)
    ramp = 0.75 + 0.5 * index.astype(jnp.float32) / PASSAGES
    values = jnp.clip(jax.random.normal(value_key, (WIDTH,), jnp.float32), -6.0, 6.0)
    return values * dense_scale * ramp


def draw_passage_lex(key, part):
    base = jax.random.fold_in(key, 11)
    indices = jnp.arange(PASSAGES)
    return jax.vmap(lambda index: lexical_row(base, index))(indices).astype(jnp.bfloat16)


def draw_passage_dense(key, part):
    base = jax.random.fold_in(key, 12)
    indices = jnp.arange(PASSAGES)
    return jax.vmap(lambda index: dense_row(base, index))(indices).astype(jnp.bfloat16)


def draw_query_lex(key, part):
    base = jax.random.fold_in(key, 21)
    mask_key, value_key = jax.random.split(base, 2)
    present = jax.random.bernoulli(mask_key, 0.25, (QUERIES, VOCAB)).astype(jnp.float32)
    values = jax.random.uniform(value_key, (QUERIES, VOCAB), jnp.float32)
    drawn = present * values * lex_scale
    return drawn.astype(jnp.bfloat16)


def draw_query_dense(key, part):
    base = jax.random.fold_in(key, 22)
    value_key = jax.random.fold_in(base, 0)
    drawn = jnp.clip(jax.random.normal(value_key, (QUERIES, WIDTH), jnp.float32), -6.0, 6.0) * dense_scale
    return drawn.astype(jnp.bfloat16)


def place_ends(values, own_key, smallest, high):
    longest = values.shape.index(max(values.shape))
    spots = []
    for shift in (0, 1):
        where = [jax.random.randint(jax.random.fold_in(own_key, axis), (), 0, length) for axis, length in enumerate(values.shape)]
        where[longest] = (where[longest] + shift) % values.shape[longest]
        spots.append(tuple(where))
    return values.at[spots[0]].set(smallest).at[spots[1]].set(high)


def setup_inputs(seed: int = 0) -> dict:
    splits = jax.random.split(jax.random.key(seed), 6)
    return {
        "query_lex": draw_query_lex(jax.random.fold_in(splits[5], 71), 0),
        "query_dense": draw_query_dense(jax.random.fold_in(splits[5], 71), 0),
        "passage_lex": draw_passage_lex(jax.random.fold_in(splits[5], 71), 0),
        "passage_dense": draw_passage_dense(jax.random.fold_in(splits[5], 71), 0),
        "positives": place_ends(jax.random.randint(splits[4], (QUERIES,), 0, PASSAGES), jax.random.fold_in(splits[4], 1), 0, PASSAGES - 1).astype(jnp.int32),
    }


def softmax_parts(logits):
    largest = jnp.max(logits, axis=1, keepdims=True)
    total = jnp.sum(jnp.exp(logits - largest), axis=1, keepdims=True)
    log_total = largest + jnp.log(total)
    return log_total[:, 0], jnp.exp(logits - log_total)


def reference(query_lex, query_dense, passage_lex, passage_dense, positives):
    lexical = jnp.dot(query_lex, passage_lex.T, preferred_element_type=jnp.float32)
    dense = jnp.dot(query_dense, passage_dense.T, preferred_element_type=jnp.float32)
    joined = dense + 0.3 * lexical
    columns = lax.broadcasted_iota(jnp.int32, (1, lexical.shape[1]), 1)
    target = (positives.astype(jnp.int32)[:, None] == columns).astype(jnp.float32)
    lse_joined, prob_joined = softmax_parts(joined)
    lse_dense, prob_dense = softmax_parts(dense)
    lse_lexical, prob_lexical = softmax_parts(lexical)
    pick_joined = jnp.sum(target * joined, axis=1)
    pick_dense = jnp.sum(target * dense, axis=1)
    pick_lexical = jnp.sum(target * lexical, axis=1)
    kl_dense = jnp.sum(prob_joined * (joined - dense), axis=1) - lse_joined + lse_dense
    kl_lex = jnp.sum(prob_joined * (joined - lexical), axis=1) - lse_joined + lse_lexical
    loss_rows = (lse_joined - pick_joined) + 0.5 * (lse_dense - pick_dense) + 0.5 * (lse_lexical - pick_lexical) + 0.5 * kl_dense + 0.5 * kl_lex
    grad_dense = (0.5 * prob_joined + prob_dense - 1.5 * target).astype(jnp.bfloat16)
    grad_lex = (-0.2 * prob_joined + prob_lexical - 0.8 * target).astype(jnp.bfloat16)
    grad_query_lex = jnp.dot(grad_lex, passage_lex, preferred_element_type=jnp.float32)
    grad_query_dense = jnp.dot(grad_dense, passage_dense, preferred_element_type=jnp.float32)
    grad_passage_lex = jnp.dot(grad_lex.T, query_lex, preferred_element_type=jnp.float32)
    grad_passage_dense = jnp.dot(grad_dense.T, query_dense, preferred_element_type=jnp.float32)
    return loss_rows, grad_query_lex, grad_query_dense, grad_passage_lex, grad_passage_dense
```

```python
import jax
import jax.numpy as jnp
from jax import lax
from jax.sharding import PartitionSpec as P


def contract_rows(first, second):
    return lax.dot_general(
        first, second, (((1,), (1,)), ((), ())), preferred_element_type=jnp.float32
    )


def contract_columns(first, second):
    return lax.dot_general(
        first, second, (((0,), (0,)), ((), ())), preferred_element_type=jnp.float32
    )


def turn(count, step):
    return [(i, (i + step) % count) for i in range(count)]


def from_chip(rows):
    count = lax.axis_size("grp")
    pieces = [rows]
    for step in range(1, count):
        pieces.append(lax.ppermute(rows, "grp", turn(count, step)))
    return jnp.concatenate(pieces, axis=0)


def on_device(query_lex, query_dense, passage_lex, passage_dense, positives):
    chip_passage_lex = from_chip(passage_lex)
    chip_passage_dense = from_chip(passage_dense)
    lex_partial = contract_rows(query_lex, passage_lex)
    dense_partial = contract_rows(query_dense, passage_dense)
    red_count = lax.axis_size("red")
    red_place = lax.axis_index("red")
    own_queries = query_lex.shape[0] // red_count
    local_passages = passage_lex.shape[0]
    first_column = lax.axis_index(("pass", "grp")) * local_passages
    lexical, dense_logit = (
        lax.psum_scatter(lex_partial, "red", scatter_dimension=0, tiled=True),
        lax.psum_scatter(dense_partial, "red", scatter_dimension=0, tiled=True),
    )
    first_query = red_place * own_queries
    query_count = lexical.shape[0]
    targets = lax.dynamic_slice_in_dim(positives, first_query, query_count)
    columns = first_column + lax.broadcasted_iota(jnp.int32, (1, local_passages), 1)
    target_mask = (targets[:, None] == columns).astype(jnp.float32)
    joined_logit = dense_logit + 0.3 * lexical
    scores = (joined_logit, dense_logit, lexical)
    local_max = tuple((jnp.max(logits, axis=1) for logits in scores))
    powers = tuple((jnp.exp(scores[slot] - local_max[slot][:, None]) for slot in range(3)))
    stats = jnp.stack(
        local_max
        + tuple((jnp.sum(power, axis=1) for power in powers))
        + (
            jnp.sum(powers[0] * (joined_logit - dense_logit), axis=1),
            jnp.sum(powers[0] * (joined_logit - lexical), axis=1),
        )
        + tuple((jnp.sum(target_mask * logits, axis=1) for logits in scores))
    )
    everyone = lax.all_gather(stats, ("pass", "grp"), axis=0)
    maxima = jnp.max(everyone[:, 0:3], axis=0)
    factors = jnp.exp(everyone[:, 0:3] - maxima)
    totals = jnp.sum(factors * everyone[:, 3:6], axis=0)
    weighted = jnp.sum(factors[:, 0:1] * everyone[:, 6:8], axis=0)
    picked_all = jnp.sum(everyone[:, 8:11], axis=0)
    log_totals = tuple((maxima[slot] + jnp.log(totals[slot]) for slot in range(3)))
    probability = tuple((jnp.exp(scores[slot] - log_totals[slot][:, None]) for slot in range(3)))
    kl_dense = weighted[0] / totals[0] - log_totals[0] + log_totals[1]
    kl_lex = weighted[1] / totals[0] - log_totals[0] + log_totals[2]
    loss_rows = (
        log_totals[0]
        - picked_all[0]
        + 0.5 * (log_totals[1] - picked_all[1])
        + 0.5 * (log_totals[2] - picked_all[2])
        + 0.5 * kl_dense
        + 0.5 * kl_lex
    )
    grad_dense = (0.5 * probability[0] + probability[1] - 1.5 * target_mask).astype(jnp.bfloat16)
    grad_lex = (-0.2 * probability[0] + probability[2] - 0.8 * target_mask).astype(jnp.bfloat16)
    grad_dense, grad_lex = (
        lax.all_gather(grad_dense, "red", axis=0, tiled=True),
        lax.all_gather(grad_lex, "red", axis=0, tiled=True),
    )
    pass_count = lax.axis_size("pass")
    pass_place = lax.axis_index("pass")
    grp_count = lax.axis_size("grp")
    grp_place = lax.axis_index("grp")
    block = query_lex.shape[0] // (pass_count * grp_count)

    def for_core(grads, core):
        blocks = grads.reshape(pass_count, grp_count, block, grads.shape[1])
        return lax.dynamic_index_in_dim(blocks, core, 1, keepdims=False)

    def with_chip(grads):
        pieces = [for_core(grads, grp_place)]
        for step in range(1, grp_count):
            away = for_core(grads, lax.rem(grp_place + step, grp_count))
            pieces.append(lax.ppermute(away, "grp", turn(grp_count, step)))
        return jnp.concatenate(pieces, axis=2)

    chip_lex = with_chip(grad_lex)
    chip_dense = with_chip(grad_dense)

    def query_terms(place):
        return (
            jnp.dot(
                lax.dynamic_index_in_dim(chip_lex, place, 0, keepdims=False),
                chip_passage_lex,
                preferred_element_type=jnp.float32,
            ),
            jnp.dot(
                lax.dynamic_index_in_dim(chip_dense, place, 0, keepdims=False),
                chip_passage_dense,
                preferred_element_type=jnp.float32,
            ),
        )

    power_of_two = pass_count & (pass_count - 1) == 0
    leaving = []
    for step in reversed(range(1, pass_count)):
        place = (
            lax.bitwise_xor(pass_place, step)
            if power_of_two
            else lax.rem(pass_place + step, pass_count)
        )
        perm = (
            [(i, i ^ step) for i in range(pass_count)]
            if power_of_two
            else [(i, (i + step) % pass_count) for i in range(pass_count)]
        )
        terms = tuple(term.astype(jnp.bfloat16) for term in query_terms(place))
        leaving.append((terms, perm))
    sent = tuple(terms for terms, _ in leaving)
    sent, grad_lex, grad_dense, chip_lex, chip_dense = lax.optimization_barrier(
        (sent, grad_lex, grad_dense, chip_lex, chip_dense)
    )
    arrived = [
        tuple(lax.ppermute(term, "pass", perm) for term in terms)
        for terms, (_, perm) in zip(sent, leaving)
    ]
    grad_passage_lex = contract_columns(grad_lex, query_lex)
    grad_passage_dense = contract_columns(grad_dense, query_dense)
    grad_query_lex, grad_query_dense = query_terms(pass_place)
    for term_lex, term_dense in arrived:
        grad_query_lex = grad_query_lex + term_lex.astype(jnp.float32)
        grad_query_dense = grad_query_dense + term_dense.astype(jnp.float32)
    return (
        loss_rows,
        grad_query_lex,
        grad_query_dense,
        grad_passage_lex,
        grad_passage_dense,
    )


def solution(mesh):
    return jax.shard_map(
        on_device,
        mesh=mesh,
        in_specs=(
            P(None, "red"),
            P(None, "red"),
            P(("pass", "grp"), "red"),
            P(("pass", "grp"), "red"),
            P(),
        ),
        out_specs=(
            P("red"),
            P(("pass", "grp"), "red"),
            P(("pass", "grp"), "red"),
            P(("pass", "grp"), "red"),
            P(("pass", "grp"), "red"),
        ),
        check_vma=False,
    )
```
